32 devices in a mesh: trial: 4 (over y, x), dp: 4 (over z), tp: 2 (over core).
Axes of the slice: x: 2, y: 2, z: 4, core: 2. Of those that a mesh axis runs over, the one named last changes fastest.
Arguments:
- slope_query: float32 [16, 768, 768], P(('trial', 'dp'), None, 'tp'), parts along dimension 0, may hold values from -4 to 4
- slope_key: float32 [16, 768, 768], P(('trial', 'dp'), None, 'tp'), parts along dimension 0, may hold values from -4 to 4
- slope_value: float32 [16, 768, 768], P(('trial', 'dp'), None, 'tp'), parts along dimension 0, may hold values from -4 to 4
- slope_mixed: float32 [16, 768, 768], P(('trial', 'dp'), 'tp'), parts along dimension 0, may hold values from -4 to 4
- slope_norm: float32 [16, 768], P(('trial', 'dp')), parts along dimension 0, may hold values from -8 to 8
- slope_bias: float32 [16, 768], P(('trial', 'dp')), parts along dimension 0, may hold values from -8 to 8
- param_query: float32 [3072, 768], P(('trial', 'dp'), 'tp'), parts along dimension 0, may hold values from -0.3125 to 0.3125
- param_key: float32 [3072, 768], P(('trial', 'dp'), 'tp'), parts along dimension 0, may hold values from -0.3125 to 0.3125
- param_value: float32 [3072, 768], P(('trial', 'dp'), 'tp'), parts along dimension 0, may hold values from -0.3125 to 0.3125
- param_mixed: float32 [3072, 768], P(('trial', 'tp'), 'dp'), parts along dimension 0, may hold values from -0.3125 to 0.3125
- param_norm: float32 [3072], P(('trial', 'dp')), parts along dimension 0, may hold values from 0.25 to 1.75
- param_bias: float32 [3072], P(('trial', 'dp')), parts along dimension 0, may hold values from -3 to 3
- state_query: float32 [3072, 768], P(('trial', 'dp'), 'tp'), parts along dimension 0, may hold values from 0.00026041668 to 0.0026041667
- state_key: float32 [3072, 768], P(('trial', 'dp'), 'tp'), parts along dimension 0, may hold values from 0.00026041668 to 0.0026041667
- state_value: float32 [3072, 768], P(('trial', 'dp'), 'tp'), parts along dimension 0, may hold values from 0.00026041668 to 0.0026041667
- state_mixed: float32 [3072, 768], P(('trial', 'tp'), 'dp'), parts along dimension 0, may hold values from 0.00026041668 to 0.0026041667
- state_norm: float32 [3072], P(('trial', 'dp')), parts along dimension 0, may hold values from 0.05 to 0.8
- state_bias: float32 [3072], P(('trial', 'dp')), parts along dimension 0, may hold values from 0.05 to 0.8
Outputs:
- half_query: bfloat16 [3072, 768], P('trial', 'tp'), parts along dimension 0
- half_key: bfloat16 [3072, 768], P('trial', 'tp'), parts along dimension 0
- half_value: bfloat16 [3072, 768], P('trial', 'tp'), parts along dimension 0
- half_mixed: bfloat16 [3072, 768], P(('trial', 'tp')), parts along dimension 0
- half_norm: bfloat16 [3072], P('trial'), parts along dimension 0
- half_bias: bfloat16 [3072], P('trial'), parts along dimension 0
- next_query: float32 [3072, 768], P(('trial', 'dp'), 'tp'), parts along dimension 0
- next_key: float32 [3072, 768], P(('trial', 'dp'), 'tp'), parts along dimension 0
- next_value: float32 [3072, 768], P(('trial', 'dp'), 'tp'), parts along dimension 0
- next_mixed: float32 [3072, 768], P(('trial', 'tp'), 'dp'), parts along dimension 0
- next_norm: float32 [3072], P(('trial', 'dp')), parts along dimension 0
- next_bias: float32 [3072], P(('trial', 'dp')), parts along dimension 0
- state_new_query: float32 [3072, 768], P(('trial', 'dp'), 'tp'), parts along dimension 0
- state_new_key: float32 [3072, 768], P(('trial', 'dp'), 'tp'), parts along dimension 0
- state_new_value: float32 [3072, 768], P(('trial', 'dp'), 'tp'), parts along dimension 0
- state_new_mixed: float32 [3072, 768], P(('trial', 'tp'), 'dp'), parts along dimension 0
- state_new_norm: float32 [3072], P(('trial', 'dp')), parts along dimension 0
- state_new_bias: float32 [3072], P(('trial', 'dp')), parts along dimension 0
The draws below stay inside these ranges and needn't reach their ends.
There are 4 independent parts, one for each index of `trial`. The reference program is written for one: setup_inputs(seed, part) draws one part's arguments, and reference() takes and returns one part's arrays. A program takes and returns all parts, laid end to end along the dimension named above; each array names one. Nothing has to cross between parts.
All inputs are finite; a program needn't handle non-finite values.
Results may differ from the reference program's by a relative error of at most 0.001.
Values may be sent and summed in bfloat16 or wider, within the bound.
A program may use at most 64 MiB of HBM per device.

```python
import jax
import jax.numpy as jnp
from jax import lax

WIDTH = 768
ATTN = 768
REPLICAS = 4


def with_spikes(entries, rng, source, target, parts, factor):
    owner, partner = [(jnp.arange(entries.shape[position]) // (entries.shape[position] // parts)).reshape([-1 if axis == position else 1 for axis in range(entries.ndim)]) for position in (source, target)]
    chosen = jax.random.permutation(rng, parts)[partner]
    strong = (owner == chosen) | (owner == (partner + parts // 2) % parts)
    return jnp.where(strong, factor * entries, entries)


def steps_of(stream_key, shape, split, low, top_value):
    gain = 1.0
    for axis_at, blocks in split:
        steps = jax.random.uniform(jax.random.fold_in(jax.random.fold_in(stream_key, 6), axis_at), (blocks,), jnp.float32, low / len(split), top_value / len(split))
        gain = gain * jnp.repeat(jnp.exp(steps), shape[axis_at] // blocks).reshape((-1,) + (1,) * (len(shape) - 1 - axis_at))
    return gain


def gaussian(rng, extent, scale, most, cuts=(), dtype=jnp.bfloat16):
    factor_of = steps_of(rng, extent, cuts, -0.22, 0.18) if cuts else 1.0
    result = jax.random.normal(rng, extent, jnp.float32) * scale * factor_of
    return jnp.minimum(jnp.maximum(result, -most), most).astype(dtype)


def gaussian_with(key, dims, width, most, shards, heavy, held_as=jnp.bfloat16):
    values = width * jax.random.normal(key, dims, jnp.float32)
    if shards:
        values = values * steps_of(key, dims, shards, -0.22, 0.18)
    return jnp.clip(with_spikes(values, jax.random.fold_in(key, 3), *heavy), -most, most).astype(held_as)


def setup_inputs(seed: int = 0, part: int = 0) -> dict:
    streams_of = jax.random.split(jax.random.key(seed), 19)
    part_splits = jax.random.split(jax.random.fold_in(streams_of[18], part), 19)
    return {
        "slope_query": gaussian_with(part_splits[0], (REPLICAS, WIDTH, ATTN), 0.5, 4.0, ((0, 4), (2, 2)), (0, 1, 4, 2.0), jnp.float32),
        "slope_key": gaussian_with(part_splits[1], (REPLICAS, WIDTH, ATTN), 0.5, 4.0, ((0, 4), (2, 2)), (0, 1, 4, 2.0), jnp.float32),
        "slope_value": gaussian_with(part_splits[2], (REPLICAS, WIDTH, ATTN), 0.5, 4.0, ((0, 4), (2, 2)), (0, 1, 4, 2.0), jnp.float32),
        "slope_mixed": gaussian_with(part_splits[3], (REPLICAS, ATTN, WIDTH), 0.5, 4.0, ((0, 4), (1, 2)), (0, 2, 4, 2.0), jnp.float32),
        "slope_norm": gaussian_with(part_splits[4], (REPLICAS, WIDTH), 1.0, 8.0, ((0, 4),), (0, 1, 4, 2.0), jnp.float32),
        "slope_bias": gaussian_with(part_splits[5], (REPLICAS, WIDTH), 1.0, 8.0, ((0, 4),), (0, 1, 4, 2.0), jnp.float32),
        "param_query": gaussian_with(part_splits[6], (WIDTH, ATTN), WIDTH ** -0.5, 0.3125, ((0, 4), (1, 2)), (1, 0, 4, 2.0), jnp.float32),
        "param_key": gaussian_with(part_splits[7], (WIDTH, ATTN), WIDTH ** -0.5, 0.3125, ((0, 4), (1, 2)), (1, 0, 4, 2.0), jnp.float32),
        "param_value": gaussian_with(part_splits[8], (WIDTH, ATTN), WIDTH ** -0.5, 0.3125, ((0, 4), (1, 2)), (1, 0, 4, 2.0), jnp.float32),
        "param_mixed": gaussian_with(part_splits[9], (ATTN, WIDTH), ATTN ** -0.5, 0.3125, ((0, 2), (1, 4)), (0, 1, 4, 2.0), jnp.float32),
        "param_norm": jnp.clip(1.0 + 0.15 * jax.random.normal(part_splits[10], (WIDTH,), jnp.float32), 0.25, 1.75),
        "param_bias": gaussian(part_splits[11], (WIDTH,), 0.5, 3.0, ((0, 4),), jnp.float32),
        "state_query": jnp.clip(0.00026041668 + 0.00234375 * jax.random.uniform(part_splits[12], (WIDTH, ATTN), jnp.float32) ** steps_of(part_splits[12], (WIDTH, ATTN), ((0, 4), (1, 2)), -0.2, 0.2), 0.00026041668, 0.0026041667),
        "state_key": jnp.clip(0.00026041668 + 0.00234375 * jax.random.uniform(part_splits[13], (WIDTH, ATTN), jnp.float32) ** steps_of(part_splits[13], (WIDTH, ATTN), ((0, 4), (1, 2)), -0.2, 0.2), 0.00026041668, 0.0026041667),
        "state_value": jnp.clip(0.00026041668 + 0.00234375 * jax.random.uniform(part_splits[14], (WIDTH, ATTN), jnp.float32) ** steps_of(part_splits[14], (WIDTH, ATTN), ((0, 4), (1, 2)), -0.2, 0.2), 0.00026041668, 0.0026041667),
        "state_mixed": jnp.clip(0.00026041668 + 0.00234375 * jax.random.uniform(part_splits[15], (ATTN, WIDTH), jnp.float32) ** steps_of(part_splits[15], (ATTN, WIDTH), ((0, 2), (1, 4)), -0.2, 0.2), 0.00026041668, 0.0026041667),
        "state_norm": jnp.clip(0.05 + 0.75 * jax.random.uniform(part_splits[16], (WIDTH,), jnp.float32) ** steps_of(part_splits[16], (WIDTH,), ((0, 4),), -0.2, 0.2), 0.05, 0.8),
        "state_bias": jnp.clip(0.05 + 0.75 * jax.random.uniform(part_splits[17], (WIDTH,), jnp.float32) ** steps_of(part_splits[17], (WIDTH,), ((0, 4),), -0.2, 0.2), 0.05, 0.8),
    }


learn_rate = 0.02
hold_rate = 0.8

def reference(slope_query, slope_key, slope_value, slope_mixed, slope_norm, slope_bias, param_query, param_key, param_value, param_mixed, param_norm, param_bias, state_query, state_key, state_value, state_mixed, state_norm, state_bias):
    mean_query = lax.optimization_barrier(jnp.sum(slope_query.astype(jnp.float32), axis=0)) * REPLICAS ** (-0.5)
    mean_key = lax.optimization_barrier(jnp.sum(slope_key.astype(jnp.float32), axis=0)) * REPLICAS ** (-0.5)
    mean_value = lax.optimization_barrier(jnp.sum(slope_value.astype(jnp.float32), axis=0)) * REPLICAS ** (-0.5)
    mean_mixed = lax.optimization_barrier(jnp.sum(slope_mixed.astype(jnp.float32), axis=0)) * REPLICAS ** (-0.5)
    mean_norm = lax.optimization_barrier(jnp.sum(slope_norm.astype(jnp.float32), axis=0)) * REPLICAS ** (-0.5)
    mean_bias = lax.optimization_barrier(jnp.sum(slope_bias.astype(jnp.float32), axis=0)) * REPLICAS ** (-0.5)
    ratio_query = jnp.sqrt(lax.optimization_barrier(jnp.sum(param_query * param_query, axis=1, keepdims=True))) * lax.rsqrt(lax.optimization_barrier(jnp.sum(mean_query * mean_query, axis=1, keepdims=True)) + 1e-06)
    mean_query = mean_query * ratio_query
    ratio_key = jnp.sqrt(lax.optimization_barrier(jnp.sum(param_key * param_key, axis=1, keepdims=True))) * lax.rsqrt(lax.optimization_barrier(jnp.sum(mean_key * mean_key, axis=1, keepdims=True)) + 1e-06)
    mean_key = mean_key * ratio_key
    ratio_value = jnp.sqrt(lax.optimization_barrier(jnp.sum(param_value * param_value, axis=1, keepdims=True))) * lax.rsqrt(lax.optimization_barrier(jnp.sum(mean_value * mean_value, axis=1, keepdims=True)) + 1e-06)
    mean_value = mean_value * ratio_value
    ratio_mixed = jnp.sqrt(lax.optimization_barrier(jnp.sum(param_mixed * param_mixed, axis=0, keepdims=True))) * lax.rsqrt(lax.optimization_barrier(jnp.sum(mean_mixed * mean_mixed, axis=0, keepdims=True)) + 1e-06)
    mean_mixed = mean_mixed * ratio_mixed
    state_new_query = hold_rate * state_query + (1.0 - hold_rate) * mean_query * mean_query
    next_query = param_query - learn_rate * mean_query * lax.rsqrt(state_new_query + 1e-06)
    state_new_key = hold_rate * state_key + (1.0 - hold_rate) * mean_key * mean_key
    next_key = param_key - learn_rate * mean_key * lax.rsqrt(state_new_key + 1e-06)
    state_new_value = hold_rate * state_value + (1.0 - hold_rate) * mean_value * mean_value
    next_value = param_value - learn_rate * mean_value * lax.rsqrt(state_new_value + 1e-06)
    state_new_mixed = hold_rate * state_mixed + (1.0 - hold_rate) * mean_mixed * mean_mixed
    next_mixed = param_mixed - learn_rate * mean_mixed * lax.rsqrt(state_new_mixed + 1e-06)
    state_new_norm = hold_rate * state_norm + (1.0 - hold_rate) * mean_norm * mean_norm
    next_norm = param_norm - learn_rate * mean_norm * lax.rsqrt(state_new_norm + 1e-06)
    state_new_bias = hold_rate * state_bias + (1.0 - hold_rate) * mean_bias * mean_bias
    next_bias = param_bias - learn_rate * mean_bias * lax.rsqrt(state_new_bias + 1e-06)
    half_query = next_query.astype(jnp.bfloat16)
    half_key = next_key.astype(jnp.bfloat16)
    half_value = next_value.astype(jnp.bfloat16)
    half_mixed = next_mixed.astype(jnp.bfloat16)
    half_norm = next_norm.astype(jnp.bfloat16)
    half_bias = next_bias.astype(jnp.bfloat16)
    return (half_query, half_key, half_value, half_mixed, half_norm, half_bias, next_query, next_key, next_value, next_mixed, next_norm, next_bias, state_new_query, state_new_key, state_new_value, state_new_mixed, state_new_norm, state_new_bias)
```

```python
import functools

import jax
import jax.numpy as jnp
from jax import lax
from jax.experimental import pallas as pl
from jax.experimental.pallas import tpu as pltpu
from jax.sharding import PartitionSpec as P

learn_rate = 0.02
hold_rate = 0.8


def shards(
    slope_query,
    slope_key,
    slope_value,
    slope_mixed,
    slope_norm,
    slope_bias,
    param_query,
    param_key,
    param_value,
    param_mixed,
    param_norm,
    param_bias,
    state_query,
    state_key,
    state_value,
    state_mixed,
    state_norm,
    state_bias,
):
    mean_query, mean_key, mean_value, mean_mixed = (
        lax.psum_scatter(slope_query[0], "dp", scatter_dimension=0, tiled=True),
        lax.psum_scatter(slope_key[0], "dp", scatter_dimension=0, tiled=True),
        lax.psum_scatter(slope_value[0], "dp", scatter_dimension=0, tiled=True),
        lax.psum_scatter(slope_mixed[0], "dp", scatter_dimension=1, tiled=True),
    )
    whole_norm, whole_bias = lax.psum((slope_norm[0], slope_bias[0]), "dp")
    place = lax.axis_index("dp")
    mean_norm = lax.dynamic_slice_in_dim(
        whole_norm, place * param_norm.shape[0], param_norm.shape[0]
    )
    mean_bias = lax.dynamic_slice_in_dim(
        whole_bias, place * param_bias.shape[0], param_bias.shape[0]
    )
    mean_rate = lax.axis_size("dp") ** (-0.5)
    mean_query = mean_query * mean_rate
    mean_key = mean_key * mean_rate
    mean_value = mean_value * mean_rate
    mean_mixed = mean_mixed * mean_rate
    mean_norm = mean_norm * mean_rate
    mean_bias = mean_bias * mean_rate
    (
        own_query,
        own_key,
        own_value,
        own_mixed,
        slope_query_norm,
        slope_key_norm,
        slope_value_norm,
        slope_mixed_norm,
    ) = lax.psum(
        (
            jnp.sum(param_query * param_query, axis=1, keepdims=True),
            jnp.sum(param_key * param_key, axis=1, keepdims=True),
            jnp.sum(param_value * param_value, axis=1, keepdims=True),
            jnp.sum(param_mixed * param_mixed, axis=0, keepdims=True),
            jnp.sum(mean_query * mean_query, axis=1, keepdims=True),
            jnp.sum(mean_key * mean_key, axis=1, keepdims=True),
            jnp.sum(mean_value * mean_value, axis=1, keepdims=True),
            jnp.sum(mean_mixed * mean_mixed, axis=0, keepdims=True),
        ),
        "tp",
    )
    mean_query = mean_query * (jnp.sqrt(own_query) * lax.rsqrt(slope_query_norm + 1e-06))
    mean_key = mean_key * (jnp.sqrt(own_key) * lax.rsqrt(slope_key_norm + 1e-06))
    mean_value = mean_value * (jnp.sqrt(own_value) * lax.rsqrt(slope_value_norm + 1e-06))
    mean_mixed = mean_mixed * (jnp.sqrt(own_mixed) * lax.rsqrt(slope_mixed_norm + 1e-06))
    state_new_query = hold_rate * state_query + (1.0 - hold_rate) * mean_query * mean_query
    next_query = param_query - learn_rate * mean_query * lax.rsqrt(state_new_query + 1e-06)
    state_new_key = hold_rate * state_key + (1.0 - hold_rate) * mean_key * mean_key
    next_key = param_key - learn_rate * mean_key * lax.rsqrt(state_new_key + 1e-06)
    state_new_value = hold_rate * state_value + (1.0 - hold_rate) * mean_value * mean_value
    next_value = param_value - learn_rate * mean_value * lax.rsqrt(state_new_value + 1e-06)
    state_new_mixed = hold_rate * state_mixed + (1.0 - hold_rate) * mean_mixed * mean_mixed
    next_mixed = param_mixed - learn_rate * mean_mixed * lax.rsqrt(state_new_mixed + 1e-06)
    state_new_norm = hold_rate * state_norm + (1.0 - hold_rate) * mean_norm * mean_norm
    next_norm = param_norm - learn_rate * mean_norm * lax.rsqrt(state_new_norm + 1e-06)
    state_new_bias = hold_rate * state_bias + (1.0 - hold_rate) * mean_bias * mean_bias
    next_bias = param_bias - learn_rate * mean_bias * lax.rsqrt(state_new_bias + 1e-06)
    half_query, half_key, half_value, half_mixed, half_norm, half_bias = (
        lax.all_gather(next_query.astype(jnp.bfloat16), "dp", axis=0, tiled=True),
        lax.all_gather(next_key.astype(jnp.bfloat16), "dp", axis=0, tiled=True),
        lax.all_gather(next_value.astype(jnp.bfloat16), "dp", axis=0, tiled=True),
        lax.all_gather(next_mixed.astype(jnp.bfloat16), "dp", axis=1, tiled=True),
        lax.all_gather(next_norm.astype(jnp.bfloat16), "dp", axis=0, tiled=True),
        lax.all_gather(next_bias.astype(jnp.bfloat16), "dp", axis=0, tiled=True),
    )
    return (
        half_query,
        half_key,
        half_value,
        half_mixed,
        half_norm,
        half_bias,
        next_query,
        next_key,
        next_value,
        next_mixed,
        next_norm,
        next_bias,
        state_new_query,
        state_new_key,
        state_new_value,
        state_new_mixed,
        state_new_norm,
        state_new_bias,
    )


MESH = pl.DeviceIdType.MESH
GAIN = 1024.0
ORDER = (0, 3, 1, 2)
PIECES = 4
SENT = ((2, 0), (3, 0), (1, 1))
STEPS = ("G2", "N2", "F0", "G3", "N3", "A", "G0", "T")
LATE = {"N3": 0, "N2": 0, "F0": 2, "T": 1, "A": 2, "G2": 5, "G0": 16, "G3": 22}
END_LAG = 3


def plan_of(mesh):
    n, pair = mesh.shape["dp"], mesh.shape["tp"]
    return n if pair == 2 and n == 4 else None


def encode(x):
    t = x * GAIN
    t = t * t
    t = t * t
    t = t * t
    return jnp.where(x < 0, -t, t).astype(jnp.bfloat16)


def decode(y):
    y = y.astype(jnp.float32)
    fourth = lax.rsqrt(lax.rsqrt(jnp.abs(y)))
    root = fourth * lax.rsqrt(jnp.maximum(fourth, 1e-30)) * (1.0 / GAIN)
    return jnp.where(y < 0, -root, root)


def update(param, state, mean):
    state_new = hold_rate * state + (1.0 - hold_rate) * mean * mean
    return state_new, param - learn_rate * mean * lax.rsqrt(state_new + 1e-06)


def kernel(n, *refs):
    (sq, sk, sv, sm, sn, sb, pq, pk, pv, pm, pn, pb, tq, tk, tv, tm, tn, tb) = refs[:18]
    G, HM, hn, hb, NX, NS, xn, xb, nn, nb = refs[18:28]
    (X, XM, S, RN, RF, TOT, P_, T_, ES, ER, VS, VP, VR, VN, VO,
     load_sem, bulk_sem, par_sem, vec_sem, tx, rn_sem, rf_sem, ag_sem,
     e_send, e_recv, v_send, v_recv, vn_send, vn_recv) = refs[28:]
    H = PIECES
    own, W = X.shape[2:]
    rows = n * own
    B = own // H
    C = H * len(ORDER)
    me = lax.axis_index("dp")
    core = lax.axis_index("tp")
    rate = float(n) ** (-0.5)
    slopes, params, states = (sq, sk, sv, sm), (pq, pk, pv, pm), (tq, tk, tv, tm)
    low = me < n // 2
    end = jnp.logical_or(me == 0, me == n - 1)

    def ref(k):
        return jnp.where(low, k, n - 1 - k)

    near = jnp.where(end, ref(1), ref(0))
    far = ref(2)

    barrier = pltpu.get_barrier_semaphore()
    pl.semaphore_signal(barrier, inc=1, device_id={"dp": near}, device_id_type=MESH)

    @pl.when(jnp.logical_not(end))
    def _():
        pl.semaphore_signal(barrier, inc=1, device_id={"dp": far}, device_id_type=MESH)

    pl.semaphore_signal(barrier, inc=1, device_id={"tp": 1 - core}, device_id_type=MESH)

    def at(c):
        return c // H, pl.ds(pl.multiple_of(lax.rem(c, H) * B, 16), B)

    def load(h):
        part = pl.ds(pl.multiple_of(h * B, 16), B)
        return pltpu.make_async_copy(slopes[ORDER[0]].at[:, part], X.at[0, :, part], load_sem.at[h])

    bulk = [
        pltpu.make_async_copy(sm.at[0], XM, bulk_sem.at[k]) if m == 3
        else pltpu.make_async_copy(slopes[m], X.at[k], bulk_sem.at[k])
        for k, m in enumerate(ORDER)
        if k
    ]
    pars = [
        pltpu.make_async_copy(src[m], dst.at[k], par_sem.at[i, k])
        for k, m in enumerate(ORDER)
        for i, (src, dst) in enumerate(((params, P_), (states, T_)))
    ]
    for h in range(H):
        load(h).start()

    def vec_loads(three):
        return [
            pltpu.make_async_copy(three[0], VS, vec_sem.at[0]),
            pltpu.make_async_copy(three[1], VP.at[0], vec_sem.at[1]),
            pltpu.make_async_copy(three[2], VP.at[1], vec_sem.at[2]),
        ]

    @pl.when(core == 0)
    def _():
        for cp in vec_loads((sn, pn, tn)):
            cp.start()

    @pl.when(core == 1)
    def _():
        for cp in vec_loads((sb, pb, tb)):
            cp.start()

    for cp in bulk[:1] + pars[:2] + bulk[1:] + pars[2:]:
        cp.start()

    def remote(src, dst, ss, rs, to):
        return pltpu.make_async_remote_copy(
            src_ref=src, dst_ref=dst, send_sem=ss, recv_sem=rs, device_id={"dp": to}, device_id_type=MESH
        )

    def to_near_rs(c, j):
        m, part = at(c)
        return remote(S.at[m, j, part], RF.at[m, j, part], tx.at[0], rf_sem.at[c, j], near)

    def end_to_near_rs(c, j):
        m, part = at(c)
        return remote(S.at[m, j, part], RN.at[m, j, part], tx.at[0], rn_sem.at[c, j], near)

    def to_far_rs(c, j):
        m, part = at(c)
        return remote(S.at[m, j, part], RF.at[m, j, part], tx.at[0], rf_sem.at[c, j], far)

    def ag(c, j, k, to):
        m, part = at(c)
        return remote(G.at[m, j, part], G.at[m, j, part], tx.at[k], ag_sem.at[c, j], to)

    def pair(c):
        return pltpu.make_async_remote_copy(
            src_ref=ES.at[c], dst_ref=ER.at[c], send_sem=e_send, recv_sem=e_recv.at[c],
            device_id={"tp": 1 - core}, device_id_type=MESH,
        )

    def vec(j, k, to):
        return remote(VR.at[j], VR.at[j], v_send.at[k], v_recv.at[j], to)

    def vec_pair():
        return pltpu.make_async_remote_copy(
            src_ref=VN, dst_ref=VO, send_sem=vn_send, recv_sem=vn_recv,
            device_id={"tp": 1 - core}, device_id_type=MESH,
        )

    part_w = own

    def vec_start():
        for cp in vec_loads((sn, pn, tn)):
            cp.wait()
        for j in range(n):
            VR[me, j : j + 1, :part_w] = VS[:, j * part_w : (j + 1) * part_w]
        for k in range(2):
            VR[me, n + k : n + k + 1, :part_w] = VP[k]

    def vec_sum():
        total = VR[0, :n]
        for d in range(1, n):
            total = total + VR[d, :n]
        total = total * rate
        for d in range(n):
            state_new, nxt = update(VR[d, n : n + 1], VR[d, n + 1 : n + 2], total[d : d + 1])
            VN[d : d + 1] = nxt
            VN[n + d : n + d + 1] = state_new
        vec_pair().start()

    def vec_out():
        vec_pair().wait_recv()
        for k, (x_, s_, h_) in enumerate(((xn, nn, hn), (xb, nb, hb))):
            def take(blk, x_=x_, s_=s_, h_=h_):
                x_[...] = blk[pl.ds(me, 1), :part_w]
                s_[...] = blk[pl.ds(n + me, 1), :part_w]
                line = jnp.concatenate([blk[d : d + 1, :part_w] for d in range(n)], axis=1)
                h_[...] = jnp.concatenate(
                    [line[:, i * 128 : (i + 1) * 128] for i in range(rows // 128)], axis=0
                ).astype(jnp.bfloat16)

            @pl.when(core == k)
            def _(take=take):
                take(VN)

            @pl.when(core != k)
            def _(take=take):
                take(VO)

    def mixed_in():
        bulk[0].wait()
        for b in range(XM.shape[1] // 64):
            j, r = (b * 64) // own, (b * 64) % own
            if b % 2 == 0:
                t = XM[:, b * 64 : b * 64 + 128].T
            X[1, j, r : r + 64] = t[(b % 2) * 64 : (b % 2) * 64 + 64]

    def mixed_out(j):
        for b in range(rows // 128):
            @pl.when(j == b)
            def _(b=b):
                halves = [
                    G[1, r // own, r % own : r % own + 64].astype(jnp.float32)
                    for r in (b * 128, b * 128 + 64)
                ]
                HM[:, b * 128 : b * 128 + 128] = jnp.concatenate(halves, axis=0).T.astype(jnp.bfloat16)

    def sums(c, tot):
        m, part = at(c)
        mean = tot * rate
        TOT[m, part] = mean
        p = P_[m, part]
        lane = lax.broadcasted_iota(jnp.int32, (B, 128), 1)
        ES[c] = jnp.where(
            lane < 64, jnp.sum(p * p, axis=1, keepdims=True), jnp.sum(mean * mean, axis=1, keepdims=True)
        )
        pair(c).start()

    def apply(c):
        m, part = at(c)
        pair(c).wait_recv()
        both = ES[c] + ER[c]
        ratio = jnp.sqrt(both[:, :1]) * lax.rsqrt(both[:, 64:65] + 1e-06)
        state_new, nxt = update(P_[m, part], T_[m, part], TOT[m, part] * ratio)
        G[m, me, part] = nxt.astype(jnp.bfloat16)
        NX[m, part] = nxt
        NS[m, part] = state_new

    @pl.when(end)
    def _():
        pl.semaphore_wait(barrier, 2)

        def push(t, carry):
            for k, late in SENT:
                @pl.when(jnp.logical_and(t >= late, t < C + late))
                def _(k=k, late=late):
                    c, j = t - late, ref(k)
                    m, part = at(c)
                    S[m, j, part] = encode(X[m, j, part])
                    end_to_near_rs(c, j).start()

            return carry

        def first(t, carry):
            load(t).wait()
            return push(t, carry)

        lax.fori_loop(0, H, first, 0)
        vec_start()
        vec(me, 0, near).start()
        mixed_in()
        for cp in bulk[1:]:
            cp.wait()
        lax.fori_loop(H, C + max(late for _, late in SENT), push, 0)
        for cp in pars:
            cp.wait()

        def step(t, carry):
            @pl.when(t < C)
            def _():
                m, part = at(t)
                to_near_rs(t, me).wait_recv()
                sums(t, X[m, me, part] + decode(RF[m, me, part]))

            @pl.when(t >= END_LAG)
            def _():
                apply(t - END_LAG)
                ag(t - END_LAG, me, 0, near).start()

            return carry

        lax.fori_loop(0, C + END_LAG, step, 0)
        for k in range(1, n):
            vec(ref(k), 0, near).wait_recv()
        vec_sum()
        vec_out()

        def finish(c, carry):
            for k in range(1, n):
                ag(c, ref(k), 0, near).wait_recv()
            mixed_out(c - 2 * H)
            return carry

        lax.fori_loop(0, C, finish, 0)
        vec(me, 0, near).wait_send()

    @pl.when(jnp.logical_not(end))
    def _():
        pl.semaphore_wait(barrier, 3)
        vec_start()
        vec(me, 0, near).start()
        vec(me, 1, far).start()
        for h in range(H):
            load(h).wait()

        def pass_on(c, j, to, into_far):
            m, part = at(c)
            if into_far:
                end_to_near_rs(c, j).wait_recv()
                S[m, j, part] = encode(decode(RN[m, j, part]) + X[m, j, part])
                to_far_rs(c, j).start()
            else:
                to_far_rs(c, j).wait_recv()
                S[m, j, part] = encode(decode(RF[m, j, part]) + X[m, j, part])
                to_near_rs(c, j).start()

        def total(c):
            m, part = at(c)
            end_to_near_rs(c, me).wait_recv()
            to_far_rs(c, me).wait_recv()
            sums(c, X[m, me, part] + decode(RN[m, me, part]) + decode(RF[m, me, part]))

        def spread(c):
            apply(c)
            ag(c, me, 0, far).start()
            ag(c, me, 1, near).start()

        def relay(c, j, to):
            ag(c, j, 1, to).wait_recv()
            ag(c, j, 1, to).start()

        acts = {
            "N3": lambda c: pass_on(c, ref(3), far, True),
            "N2": lambda c: pass_on(c, ref(2), far, True),
            "F0": lambda c: pass_on(c, ref(0), near, False),
            "T": total,
            "A": spread,
            "G2": lambda c: relay(c, ref(2), near),
            "G0": lambda c: relay(c, ref(0), far),
            "G3": lambda c: relay(c, ref(3), near),
        }
        last = C + max(LATE.values())
        turn = last - rows // 128

        def step(t, carry):
            @pl.when(t == 1)
            def _():
                for cp in bulk[1:] + pars:
                    cp.wait()
                mixed_in()

            for name in STEPS:
                late = LATE[name]

                @pl.when(jnp.logical_and(t >= late, t < C + late))
                def _(name=name, late=late):
                    acts[name](t - late)

            @pl.when(t == 7)
            def _():
                vec(ref(0), 2, far).wait_recv()
                vec(ref(0), 2, far).start()
                vec(ref(2), 3, near).wait_recv()
                vec(ref(2), 3, near).start()

            @pl.when(t == 11)
            def _():
                vec(ref(3), 4, near).wait_recv()
                vec(ref(3), 4, near).start()
                vec_sum()

            @pl.when(t == 13)
            def _():
                vec_out()

            mixed_out(t - turn)
            return carry

        lax.fori_loop(0, last, step, 0)
        for k, (j, to) in enumerate(((me, near), (me, far), (ref(0), far), (ref(2), near), (ref(3), near))):
            vec(j, k, to).wait_send()
        remote(S, S, tx.at[1], rf_sem.at[0, 0], near).wait_send()

    remote(S, S, tx.at[0], rf_sem.at[0, 0], near).wait_send()
    pltpu.make_async_remote_copy(
        src_ref=ES, dst_ref=ER, send_sem=e_send, recv_sem=e_recv.at[0],
        device_id={"tp": 1 - core}, device_id_type=MESH,
    ).wait_send()
    vec_pair().wait_send()


def settle(n, *refs):
    G, HM, hn, hb, NX, NS, xn, xb, nn, nb = refs[:10]
    outs, sem = refs[10:28], refs[28]
    place = {m: k for k, m in enumerate(ORDER)}
    srcs = [G.at[place[m]] for m in range(3)] + [HM, hn, hb]
    srcs += [NX.at[place[m]] for m in range(4)] + [xn, xb]
    srcs += [NS.at[place[m]] for m in range(4)] + [nn, nb]
    copies = [pltpu.make_async_copy(s, d, sem.at[i]) for i, (s, d) in enumerate(zip(srcs, outs))]
    for cp in copies:
        cp.start()
    for cp in copies:
        cp.wait()


def fused(n, *args):
    slopes, params, states = list(args[:6]), list(args[6:12]), list(args[12:])
    own, width = params[0].shape
    rows = n * own
    H = PIECES
    if own % (H * 16) or own % 64 or width % 128 or rows % 128 or args[3].shape[1:] != (width, rows):
        return shards(*args)
    C, B = H * len(ORDER), own // H
    for i in range(3):
        slopes[i] = slopes[i].reshape(n, own, width)
    for group in (params, states):
        group[3] = group[3].T
        for i in (4, 5):
            group[i] = group[i].reshape(1, -1)
    hbm, vmem = pl.BlockSpec(memory_space=pltpu.HBM), pl.BlockSpec(memory_space=pltpu.VMEM)
    f32, bf16 = jnp.float32, jnp.bfloat16
    wide = -(-own // 128) * 128
    dma = pltpu.SemaphoreType.DMA
    four = len(ORDER)
    held = (
        [((four, n, own, width), bf16), ((width, rows), bf16)]
        + [((rows // 128, 128), bf16)] * 2
        + [((four, own, width), f32)] * 2
        + [((1, own), f32)] * 4
    )
    given = [pltpu.with_memory_space_constraint(x, pltpu.HBM) for x in slopes + params + states]
    blocks = pl.pallas_call(
        functools.partial(kernel, n),
        out_shape=[pltpu.VMEM(s, d) for s, d in held],
        in_specs=[hbm] * 18,
        out_specs=[vmem] * len(held),
        scratch_shapes=[
            pltpu.VMEM((four, n, own, width), f32),
            pltpu.VMEM((width, rows), f32),
            pltpu.VMEM((four, n, own, width), bf16),
            pltpu.VMEM((four, n, own, width), bf16),
            pltpu.VMEM((four, n, own, width), bf16),
            pltpu.VMEM((four, own, width), f32),
            pltpu.VMEM((four, own, width), f32),
            pltpu.VMEM((four, own, width), f32),
            pltpu.VMEM((C, B, 128), f32),
            pltpu.VMEM((C, B, 128), f32),
            pltpu.VMEM((1, rows), f32),
            pltpu.VMEM((2, 1, own), f32),
            pltpu.VMEM((n, 8, wide), f32),
            pltpu.VMEM((2 * n, wide), f32),
            pltpu.VMEM((2 * n, wide), f32),
            dma((H,)), dma((four,)), dma((2, four)), dma((3,)), dma((2,)), dma((C, n)), dma((C, n)), dma((C, n)),
            dma, dma((C,)), dma((5,)), dma((n,)), dma, dma,
        ],
        compiler_params=pltpu.CompilerParams(
            collective_id=0, has_side_effects=True, vmem_limit_bytes=48 * 2**20
        ),
        cost_estimate=pl.CostEstimate(flops=10**7, bytes_accessed=10**7, transcendentals=0),
    )(*given)
    S = jax.ShapeDtypeStruct
    final = (
        [S((n, own, width), bf16)] * 3 + [S((width, rows), bf16)] + [S((rows // 128, 128), bf16)] * 2
        + ([S((own, width), f32)] * 4 + [S((1, own), f32)] * 2) * 2
    )
    outs = list(
        pl.pallas_call(
            functools.partial(settle, n),
            out_shape=final,
            in_specs=[vmem] * len(held),
            out_specs=[hbm] * len(final),
            scratch_shapes=[dma((len(final),))],
            compiler_params=pltpu.CompilerParams(vmem_limit_bytes=2**20),
            cost_estimate=pl.CostEstimate(flops=10**6, bytes_accessed=10**7, transcendentals=0),
        )(*blocks)
    )
    for k in range(3):
        outs[k] = outs[k].reshape(rows, width)
    for k in (9, 15):
        outs[k] = outs[k].T
    for k in (4, 5, 10, 11, 16, 17):
        outs[k] = outs[k].reshape(-1)
    return tuple(outs)


def solution(mesh):
    in_specs = (
        P(("trial", "dp"), None, "tp"),
        P(("trial", "dp"), None, "tp"),
        P(("trial", "dp"), None, "tp"),
        P(("trial", "dp"), "tp", None),
        P(("trial", "dp"), None),
        P(("trial", "dp"), None),
        P(("trial", "dp"), "tp"),
        P(("trial", "dp"), "tp"),
        P(("trial", "dp"), "tp"),
        P(("trial", "tp"), "dp"),
        P(("trial", "dp")),
        P(("trial", "dp")),
        P(("trial", "dp"), "tp"),
        P(("trial", "dp"), "tp"),
        P(("trial", "dp"), "tp"),
        P(("trial", "tp"), "dp"),
        P(("trial", "dp")),
        P(("trial", "dp")),
    )
    out_specs = (
        P("trial", "tp"),
        P("trial", "tp"),
        P("trial", "tp"),
        P(("trial", "tp"), None),
        P("trial"),
        P("trial"),
        P(("trial", "dp"), "tp"),
        P(("trial", "dp"), "tp"),
        P(("trial", "dp"), "tp"),
        P(("trial", "tp"), "dp"),
        P(("trial", "dp")),
        P(("trial", "dp")),
        P(("trial", "dp"), "tp"),
        P(("trial", "dp"), "tp"),
        P(("trial", "dp"), "tp"),
        P(("trial", "tp"), "dp"),
        P(("trial", "dp")),
        P(("trial", "dp")),
    )
    plan = plan_of(mesh)
    body = shards if plan is None else functools.partial(fused, plan)
    return jax.shard_map(body, mesh=mesh, in_specs=in_specs, out_specs=out_specs, check_vma=False)
```

```python
import functools

import jax
import jax.numpy as jnp
from jax import lax
from jax.experimental import pallas as pl
from jax.experimental.pallas import tpu as pltpu
from jax.sharding import PartitionSpec as P

learn_rate = 0.02
hold_rate = 0.8


def shards(
    slope_query,
    slope_key,
    slope_value,
    slope_mixed,
    slope_norm,
    slope_bias,
    param_query,
    param_key,
    param_value,
    param_mixed,
    param_norm,
    param_bias,
    state_query,
    state_key,
    state_value,
    state_mixed,
    state_norm,
    state_bias,
):
    mean_query, mean_key, mean_value, mean_mixed = (
        lax.psum_scatter(slope_query[0], "dp", scatter_dimension=0, tiled=True),
        lax.psum_scatter(slope_key[0], "dp", scatter_dimension=0, tiled=True),
        lax.psum_scatter(slope_value[0], "dp", scatter_dimension=0, tiled=True),
        lax.psum_scatter(slope_mixed[0], "dp", scatter_dimension=1, tiled=True),
    )
    whole_norm, whole_bias = lax.psum((slope_norm[0], slope_bias[0]), "dp")
    place = lax.axis_index("dp")
    mean_norm = lax.dynamic_slice_in_dim(
        whole_norm, place * param_norm.shape[0], param_norm.shape[0]
    )
    mean_bias = lax.dynamic_slice_in_dim(
        whole_bias, place * param_bias.shape[0], param_bias.shape[0]
    )
    mean_rate = lax.axis_size("dp") ** (-0.5)
    mean_query = mean_query * mean_rate
    mean_key = mean_key * mean_rate
    mean_value = mean_value * mean_rate
    mean_mixed = mean_mixed * mean_rate
    mean_norm = mean_norm * mean_rate
    mean_bias = mean_bias * mean_rate
    (
        own_query,
        own_key,
        own_value,
        own_mixed,
        slope_query_norm,
        slope_key_norm,
        slope_value_norm,
        slope_mixed_norm,
    ) = lax.psum(
        (
            jnp.sum(param_query * param_query, axis=1, keepdims=True),
            jnp.sum(param_key * param_key, axis=1, keepdims=True),
            jnp.sum(param_value * param_value, axis=1, keepdims=True),
            jnp.sum(param_mixed * param_mixed, axis=0, keepdims=True),
            jnp.sum(mean_query * mean_query, axis=1, keepdims=True),
            jnp.sum(mean_key * mean_key, axis=1, keepdims=True),
            jnp.sum(mean_value * mean_value, axis=1, keepdims=True),
            jnp.sum(mean_mixed * mean_mixed, axis=0, keepdims=True),
        ),
        "tp",
    )
    mean_query = mean_query * (jnp.sqrt(own_query) * lax.rsqrt(slope_query_norm + 1e-06))
    mean_key = mean_key * (jnp.sqrt(own_key) * lax.rsqrt(slope_key_norm + 1e-06))
    mean_value = mean_value * (jnp.sqrt(own_value) * lax.rsqrt(slope_value_norm + 1e-06))
    mean_mixed = mean_mixed * (jnp.sqrt(own_mixed) * lax.rsqrt(slope_mixed_norm + 1e-06))
    state_new_query = hold_rate * state_query + (1.0 - hold_rate) * mean_query * mean_query
    next_query = param_query - learn_rate * mean_query * lax.rsqrt(state_new_query + 1e-06)
    state_new_key = hold_rate * state_key + (1.0 - hold_rate) * mean_key * mean_key
    next_key = param_key - learn_rate * mean_key * lax.rsqrt(state_new_key + 1e-06)
    state_new_value = hold_rate * state_value + (1.0 - hold_rate) * mean_value * mean_value
    next_value = param_value - learn_rate * mean_value * lax.rsqrt(state_new_value + 1e-06)
    state_new_mixed = hold_rate * state_mixed + (1.0 - hold_rate) * mean_mixed * mean_mixed
    next_mixed = param_mixed - learn_rate * mean_mixed * lax.rsqrt(state_new_mixed + 1e-06)
    state_new_norm = hold_rate * state_norm + (1.0 - hold_rate) * mean_norm * mean_norm
    next_norm = param_norm - learn_rate * mean_norm * lax.rsqrt(state_new_norm + 1e-06)
    state_new_bias = hold_rate * state_bias + (1.0 - hold_rate) * mean_bias * mean_bias
    next_bias = param_bias - learn_rate * mean_bias * lax.rsqrt(state_new_bias + 1e-06)
    half_query, half_key, half_value, half_mixed, half_norm, half_bias = (
        lax.all_gather(next_query.astype(jnp.bfloat16), "dp", axis=0, tiled=True),
        lax.all_gather(next_key.astype(jnp.bfloat16), "dp", axis=0, tiled=True),
        lax.all_gather(next_value.astype(jnp.bfloat16), "dp", axis=0, tiled=True),
        lax.all_gather(next_mixed.astype(jnp.bfloat16), "dp", axis=1, tiled=True),
        lax.all_gather(next_norm.astype(jnp.bfloat16), "dp", axis=0, tiled=True),
        lax.all_gather(next_bias.astype(jnp.bfloat16), "dp", axis=0, tiled=True),
    )
    return (
        half_query,
        half_key,
        half_value,
        half_mixed,
        half_norm,
        half_bias,
        next_query,
        next_key,
        next_value,
        next_mixed,
        next_norm,
        next_bias,
        state_new_query,
        state_new_key,
        state_new_value,
        state_new_mixed,
        state_new_norm,
        state_new_bias,
    )


MESH = pl.DeviceIdType.MESH
GAIN = 1024.0
ORDER = (0, 3, 1, 2)
PIECES = 4
SENT = ((2, 0), (3, 1), (1, 1))
STEPS = ('T', 'F0', 'G0', 'N2', 'G2', 'G3', 'N3', 'A')
LATE = {'N3': 1, 'N2': 0, 'F0': 3, 'T': 2, 'A': 2, 'G2': 4, 'G0': 17, 'G3': 21}
END_LAG = 2


def plan_of(mesh):
    n, pair = mesh.shape["dp"], mesh.shape["tp"]
    return n if pair == 2 and n == 4 else None


def encode(x):
    t = x * GAIN
    t = t * t
    t = t * t
    t = t * t
    return jnp.where(x < 0, -t, t).astype(jnp.bfloat16)


def decode(y):
    y = y.astype(jnp.float32)
    fourth = lax.rsqrt(lax.rsqrt(jnp.abs(y)))
    root = fourth * lax.rsqrt(jnp.maximum(fourth, 1e-30)) * (1.0 / GAIN)
    return jnp.where(y < 0, -root, root)


def update(param, state, mean):
    state_new = hold_rate * state + (1.0 - hold_rate) * mean * mean
    return state_new, param - learn_rate * mean * lax.rsqrt(state_new + 1e-06)


def kernel(n, *refs):
    (sq, sk, sv, sm, sn, sb, pq, pk, pv, pm, pn, pb, tq, tk, tv, tm, tn, tb) = refs[:18]
    G, HM, hn, hb, NX, NS, xn, xb, nn, nb = refs[18:28]
    (X, XM, S, RN, RF, TOT, P_, T_, ES, ER, VS, VP, VR, VN, VO,
     load_sem, bulk_sem, par_sem, vec_sem, tx, rn_sem, rf_sem, ag_sem,
     e_send, e_recv, v_send, v_recv, vn_send, vn_recv) = refs[28:]
    H = PIECES
    own, W = X.shape[2:]
    rows = n * own
    B = own // H
    C = H * len(ORDER)
    me = lax.axis_index("dp")
    core = lax.axis_index("tp")
    rate = float(n) ** (-0.5)
    slopes, params, states = (sq, sk, sv, sm), (pq, pk, pv, pm), (tq, tk, tv, tm)
    low = me < n // 2
    end = jnp.logical_or(me == 0, me == n - 1)

    def ref(k):
        return jnp.where(low, k, n - 1 - k)

    near = jnp.where(end, ref(1), ref(0))
    far = ref(2)

    def at(c):
        return c // H, pl.ds(pl.multiple_of(lax.rem(c, H) * B, 16), B)

    def load(h):
        part = pl.ds(pl.multiple_of(h * B, 16), B)
        return pltpu.make_async_copy(slopes[ORDER[0]].at[:, part], X.at[0, :, part], load_sem.at[h])

    bulk = [
        pltpu.make_async_copy(sm.at[0], XM, bulk_sem.at[k]) if m == 3
        else pltpu.make_async_copy(slopes[m], X.at[k], bulk_sem.at[k])
        for k, m in enumerate(ORDER)
        if k
    ]
    pars = [
        pltpu.make_async_copy(src[m], dst.at[k], par_sem.at[i, k])
        for k, m in enumerate(ORDER)
        for i, (src, dst) in enumerate(((params, P_), (states, T_)))
    ]
    load(0).start()
    barrier = pltpu.get_barrier_semaphore()
    pl.semaphore_signal(barrier, inc=1, device_id={"dp": near}, device_id_type=MESH)

    @pl.when(jnp.logical_not(end))
    def _():
        pl.semaphore_signal(barrier, inc=1, device_id={"dp": far}, device_id_type=MESH)

    pl.semaphore_signal(barrier, inc=1, device_id={"tp": 1 - core}, device_id_type=MESH)

    for h in range(1, H):
        load(h).start()

    def vec_loads(three):
        return [
            pltpu.make_async_copy(three[0], VS, vec_sem.at[0]),
            pltpu.make_async_copy(three[1], VP.at[0], vec_sem.at[1]),
            pltpu.make_async_copy(three[2], VP.at[1], vec_sem.at[2]),
        ]

    @pl.when(core == 0)
    def _():
        for cp in vec_loads((sn, pn, tn)):
            cp.start()

    @pl.when(core == 1)
    def _():
        for cp in vec_loads((sb, pb, tb)):
            cp.start()

    for cp in bulk[:1] + pars[:2] + bulk[1:] + pars[2:]:
        cp.start()

    def remote(src, dst, ss, rs, to):
        return pltpu.make_async_remote_copy(
            src_ref=src, dst_ref=dst, send_sem=ss, recv_sem=rs, device_id={"dp": to}, device_id_type=MESH
        )

    def to_near_rs(c, j):
        m, part = at(c)
        return remote(S.at[m, j, part], RF.at[m, j, part], tx.at[0], rf_sem.at[c, j], near)

    def end_to_near_rs(c, j):
        m, part = at(c)
        return remote(S.at[m, j, part], RN.at[m, j, part], tx.at[0], rn_sem.at[c, j], near)

    def to_far_rs(c, j):
        m, part = at(c)
        return remote(S.at[m, j, part], RF.at[m, j, part], tx.at[0], rf_sem.at[c, j], far)

    def ag(c, j, k, to):
        m, part = at(c)
        return remote(G.at[m, j, part], G.at[m, j, part], tx.at[k], ag_sem.at[c, j], to)

    def pair(c):
        return pltpu.make_async_remote_copy(
            src_ref=ES.at[c], dst_ref=ER.at[c], send_sem=e_send, recv_sem=e_recv.at[c],
            device_id={"tp": 1 - core}, device_id_type=MESH,
        )

    def vec(j, k, to):
        return remote(VR.at[j], VR.at[j], v_send.at[k], v_recv.at[j], to)

    def vec_pair():
        return pltpu.make_async_remote_copy(
            src_ref=VN, dst_ref=VO, send_sem=vn_send, recv_sem=vn_recv,
            device_id={"tp": 1 - core}, device_id_type=MESH,
        )

    part_w = own

    def vec_start():
        for cp in vec_loads((sn, pn, tn)):
            cp.wait()
        for j in range(n):
            VR[me, j : j + 1, :part_w] = VS[:, j * part_w : (j + 1) * part_w]
        for k in range(2):
            VR[me, n + k : n + k + 1, :part_w] = VP[k]

    def vec_sum():
        total = VR[0, :n]
        for d in range(1, n):
            total = total + VR[d, :n]
        total = total * rate
        for d in range(n):
            state_new, nxt = update(VR[d, n : n + 1], VR[d, n + 1 : n + 2], total[d : d + 1])
            VN[d : d + 1] = nxt
            VN[n + d : n + d + 1] = state_new
        vec_pair().start()

    def vec_out():
        vec_pair().wait_recv()
        for k, (x_, s_, h_) in enumerate(((xn, nn, hn), (xb, nb, hb))):
            def take(blk, x_=x_, s_=s_, h_=h_):
                x_[...] = blk[pl.ds(me, 1), :part_w]
                s_[...] = blk[pl.ds(n + me, 1), :part_w]
                line = jnp.concatenate([blk[d : d + 1, :part_w] for d in range(n)], axis=1)
                h_[...] = jnp.concatenate(
                    [line[:, i * 128 : (i + 1) * 128] for i in range(rows // 128)], axis=0
                ).astype(jnp.bfloat16)

            @pl.when(core == k)
            def _(take=take):
                take(VN)

            @pl.when(core != k)
            def _(take=take):
                take(VO)

    def mixed_in():
        bulk[0].wait()
        for b in range(XM.shape[1] // 64):
            j, r = (b * 64) // own, (b * 64) % own
            if b % 2 == 0:
                t = XM[:, b * 64 : b * 64 + 128].T
            X[1, j, r : r + 64] = t[(b % 2) * 64 : (b % 2) * 64 + 64]

    def mixed_out(j):
        for b in range(rows // 128):
            @pl.when(j == b)
            def _(b=b):
                halves = [
                    G[1, r // own, r % own : r % own + 64].astype(jnp.float32)
                    for r in (b * 128, b * 128 + 64)
                ]
                HM[:, b * 128 : b * 128 + 128] = jnp.concatenate(halves, axis=0).T.astype(jnp.bfloat16)

    def sums(c, tot):
        m, part = at(c)
        mean = tot * rate
        TOT[m, part] = mean
        p = P_[m, part]
        lane = lax.broadcasted_iota(jnp.int32, (B, 128), 1)
        ES[c] = jnp.where(
            lane < 64, jnp.sum(p * p, axis=1, keepdims=True), jnp.sum(mean * mean, axis=1, keepdims=True)
        )
        pair(c).start()

    def apply(c):
        m, part = at(c)
        pair(c).wait_recv()
        both = ES[c] + ER[c]
        ratio = jnp.sqrt(both[:, :1]) * lax.rsqrt(both[:, 64:65] + 1e-06)
        state_new, nxt = update(P_[m, part], T_[m, part], TOT[m, part] * ratio)
        G[m, me, part] = nxt.astype(jnp.bfloat16)
        NX[m, part] = nxt
        NS[m, part] = state_new

    def drain():
        remote(S, S, tx.at[0], rf_sem.at[0, 0], near).wait_send()
        pltpu.make_async_remote_copy(
            src_ref=ES, dst_ref=ER, send_sem=e_send, recv_sem=e_recv.at[0],
            device_id={"tp": 1 - core}, device_id_type=MESH,
        ).wait_send()
        vec_pair().wait_send()

    @pl.when(end)
    def _():
        pl.semaphore_wait(barrier, 2)

        def push(t, carry):
            for k, late in SENT:
                @pl.when(jnp.logical_and(t >= late, t < C + late))
                def _(k=k, late=late):
                    c, j = t - late, ref(k)
                    m, part = at(c)
                    S[m, j, part] = encode(X[m, j, part])
                    end_to_near_rs(c, j).start()

            return carry

        def first(t, carry):
            load(t).wait()
            return push(t, carry)

        lax.fori_loop(0, H, first, 0)
        vec_start()
        vec(me, 0, near).start()
        mixed_in()
        for cp in bulk[1:]:
            cp.wait()
        lax.fori_loop(H, C + max(late for _, late in SENT), push, 0)
        for cp in pars:
            cp.wait()

        def step(t, carry):
            @pl.when(t < C)
            def _():
                m, part = at(t)
                to_near_rs(t, me).wait_recv()
                sums(t, X[m, me, part] + decode(RF[m, me, part]))

            @pl.when(t >= END_LAG)
            def _():
                apply(t - END_LAG)
                ag(t - END_LAG, me, 0, near).start()

            return carry

        lax.fori_loop(0, C + END_LAG, step, 0)
        for k in range(1, n):
            vec(ref(k), 0, near).wait_recv()
        vec_sum()
        vec_out()

        def finish(c, carry):
            for k in range(1, n):
                ag(c, ref(k), 0, near).wait_recv()
            mixed_out(c - 2 * H)
            return carry

        lax.fori_loop(0, C - 1, finish, 0)
        vec(me, 0, near).wait_send()
        drain()
        finish(C - 1, 0)

    @pl.when(jnp.logical_not(end))
    def _():
        pl.semaphore_wait(barrier, 3)
        vec_start()
        vec(me, 0, near).start()
        vec(me, 1, far).start()
        for h in range(H):
            load(h).wait()

        def pass_on(c, j, to, into_far):
            m, part = at(c)
            if into_far:
                end_to_near_rs(c, j).wait_recv()
                S[m, j, part] = encode(decode(RN[m, j, part]) + X[m, j, part])
                to_far_rs(c, j).start()
            else:
                to_far_rs(c, j).wait_recv()
                S[m, j, part] = encode(decode(RF[m, j, part]) + X[m, j, part])
                to_near_rs(c, j).start()

        def total(c):
            m, part = at(c)
            end_to_near_rs(c, me).wait_recv()
            to_far_rs(c, me).wait_recv()
            sums(c, X[m, me, part] + decode(RN[m, me, part]) + decode(RF[m, me, part]))

        def spread(c):
            apply(c)
            ag(c, me, 0, far).start()
            ag(c, me, 1, near).start()

        def relay(c, j, to):
            ag(c, j, 1, to).wait_recv()
            ag(c, j, 1, to).start()

        acts = {
            "N3": lambda c: pass_on(c, ref(3), far, True),
            "N2": lambda c: pass_on(c, ref(2), far, True),
            "F0": lambda c: pass_on(c, ref(0), near, False),
            "T": total,
            "A": spread,
            "G2": lambda c: relay(c, ref(2), near),
            "G0": lambda c: relay(c, ref(0), far),
            "G3": lambda c: relay(c, ref(3), near),
        }
        last = C + max(LATE.values())
        turn = last - rows // 128

        def step(t, carry):
            @pl.when(t == 0)
            def _():
                vec(ref(2), 3, near).wait_recv()
                vec(ref(2), 3, near).start()

            @pl.when(t == 1)
            def _():
                for cp in bulk[1:] + pars:
                    cp.wait()
                mixed_in()

            for name in STEPS:
                late = LATE[name]

                @pl.when(jnp.logical_and(t >= late, t < C + late))
                def _(name=name, late=late):
                    acts[name](t - late)

            @pl.when(t == 7)
            def _():
                vec(ref(0), 2, far).wait_recv()
                vec(ref(0), 2, far).start()

            @pl.when(t == 11)
            def _():
                vec(ref(3), 4, near).wait_recv()
                vec(ref(3), 4, near).start()
                vec_sum()

            @pl.when(t == 13)
            def _():
                vec_out()

            mixed_out(t - turn)
            return carry

        lax.fori_loop(0, last, step, 0)
        for k, (j, to) in enumerate(((me, near), (me, far), (ref(0), far), (ref(2), near), (ref(3), near))):
            vec(j, k, to).wait_send()
        remote(S, S, tx.at[1], rf_sem.at[0, 0], near).wait_send()
        drain()


def settle(n, *refs):
    G, HM, hn, hb, NX, NS, xn, xb, nn, nb = refs[:10]
    outs, sem = refs[10:28], refs[28]
    place = {m: k for k, m in enumerate(ORDER)}
    srcs = [G.at[place[m]] for m in range(3)] + [HM, hn, hb]
    srcs += [NX.at[place[m]] for m in range(4)] + [xn, xb]
    srcs += [NS.at[place[m]] for m in range(4)] + [nn, nb]
    group = [0] * 4 + [3, 4] + [1] * 4 + [5, 6] + [2] * 4 + [7, 8]
    for s, d, k in zip(srcs, outs, group):
        pltpu.make_async_copy(s, d, sem.at[k]).start()
    for k, whole in enumerate((G, NX, NS, hn, hb, xn, xb, nn, nb)):
        pltpu.make_async_copy(whole, whole, sem.at[k]).wait()


def fused(n, *args):
    slopes, params, states = list(args[:6]), list(args[6:12]), list(args[12:])
    own, width = params[0].shape
    rows = n * own
    H = PIECES
    if own % (H * 16) or own % 64 or width % 128 or rows % 128 or args[3].shape[1:] != (width, rows):
        return shards(*args)
    C, B = H * len(ORDER), own // H
    for i in range(3):
        slopes[i] = slopes[i].reshape(n, own, width)
    for group in (params, states):
        group[3] = group[3].T
        for i in (4, 5):
            group[i] = group[i].reshape(1, -1)
    hbm, vmem = pl.BlockSpec(memory_space=pltpu.HBM), pl.BlockSpec(memory_space=pltpu.VMEM)
    f32, bf16 = jnp.float32, jnp.bfloat16
    wide = -(-own // 128) * 128
    dma = pltpu.SemaphoreType.DMA
    four = len(ORDER)
    held = (
        [((four, n, own, width), bf16), ((width, rows), bf16)]
        + [((rows // 128, 128), bf16)] * 2
        + [((four, own, width), f32)] * 2
        + [((1, own), f32)] * 4
    )
    given = [pltpu.with_memory_space_constraint(x, pltpu.HBM) for x in slopes + params + states]
    blocks = pl.pallas_call(
        functools.partial(kernel, n),
        out_shape=[pltpu.VMEM(s, d) for s, d in held],
        in_specs=[hbm] * 18,
        out_specs=[vmem] * len(held),
        scratch_shapes=[
            pltpu.VMEM((four, n, own, width), f32),
            pltpu.VMEM((width, rows), f32),
            pltpu.VMEM((four, n, own, width), bf16),
            pltpu.VMEM((four, n, own, width), bf16),
            pltpu.VMEM((four, n, own, width), bf16),
            pltpu.VMEM((four, own, width), f32),
            pltpu.VMEM((four, own, width), f32),
            pltpu.VMEM((four, own, width), f32),
            pltpu.VMEM((C, B, 128), f32),
            pltpu.VMEM((C, B, 128), f32),
            pltpu.VMEM((1, rows), f32),
            pltpu.VMEM((2, 1, own), f32),
            pltpu.VMEM((n, 8, wide), f32),
            pltpu.VMEM((2 * n, wide), f32),
            pltpu.VMEM((2 * n, wide), f32),
            dma((H,)), dma((four,)), dma((2, four)), dma((3,)), dma((2,)), dma((C, n)), dma((C, n)), dma((C, n)),
            dma, dma((C,)), dma((5,)), dma((n,)), dma, dma,
        ],
        compiler_params=pltpu.CompilerParams(
            collective_id=0, has_side_effects=True, vmem_limit_bytes=48 * 2**20
        ),
        cost_estimate=pl.CostEstimate(flops=10**7, bytes_accessed=10**7, transcendentals=0),
    )(*given)
    S = jax.ShapeDtypeStruct
    final = (
        [S((n, own, width), bf16)] * 3 + [S((width, rows), bf16)] + [S((rows // 128, 128), bf16)] * 2
        + ([S((own, width), f32)] * 4 + [S((1, own), f32)] * 2) * 2
    )
    outs = list(
        pl.pallas_call(
            functools.partial(settle, n),
            out_shape=final,
            in_specs=[vmem] * len(held),
            out_specs=[hbm] * len(final),
            scratch_shapes=[dma((len(held) - 1,))],
            compiler_params=pltpu.CompilerParams(vmem_limit_bytes=2**20),
            cost_estimate=pl.CostEstimate(flops=10**6, bytes_accessed=10**7, transcendentals=0),
        )(*blocks)
    )
    for k in range(3):
        outs[k] = outs[k].reshape(rows, width)
    for k in (9, 15):
        outs[k] = outs[k].T
    for k in (4, 5, 10, 11, 16, 17):
        outs[k] = outs[k].reshape(-1)
    return tuple(outs)


def solution(mesh):
    in_specs = (
        P(("trial", "dp"), None, "tp"),
        P(("trial", "dp"), None, "tp"),
        P(("trial", "dp"), None, "tp"),
        P(("trial", "dp"), "tp", None),
        P(("trial", "dp"), None),
        P(("trial", "dp"), None),
        P(("trial", "dp"), "tp"),
        P(("trial", "dp"), "tp"),
        P(("trial", "dp"), "tp"),
        P(("trial", "tp"), "dp"),
        P(("trial", "dp")),
        P(("trial", "dp")),
        P(("trial", "dp"), "tp"),
        P(("trial", "dp"), "tp"),
        P(("trial", "dp"), "tp"),
        P(("trial", "tp"), "dp"),
        P(("trial", "dp")),
        P(("trial", "dp")),
    )
    out_specs = (
        P("trial", "tp"),
        P("trial", "tp"),
        P("trial", "tp"),
        P(("trial", "tp"), None),
        P("trial"),
        P("trial"),
        P(("trial", "dp"), "tp"),
        P(("trial", "dp"), "tp"),
        P(("trial", "dp"), "tp"),
        P(("trial", "tp"), "dp"),
        P(("trial", "dp")),
        P(("trial", "dp")),
        P(("trial", "dp"), "tp"),
        P(("trial", "dp"), "tp"),
        P(("trial", "dp"), "tp"),
        P(("trial", "tp"), "dp"),
        P(("trial", "dp")),
        P(("trial", "dp")),
    )
    plan = plan_of(mesh)
    body = shards if plan is None else functools.partial(fused, plan)
    return jax.shard_map(body, mesh=mesh, in_specs=in_specs, out_specs=out_specs, check_vma=False)
```
